128 devices in a mesh: dp: 1, tp: 16 (over z, y), sp: 8 (over x, core).
Axes of the slice: x: 4, y: 4, z: 4, core: 2. Of those that a mesh axis runs over, the one named last changes fastest.
Arguments:
- tokens: bfloat16 [24, 1024, 4096], P('dp', 'sp')
- attn_gain: float32 [4096], replicated
- w_qkv: bfloat16 [4096, 3, 32, 128], P(None, None, 'tp')
- w_rel: bfloat16 [4096, 32, 128], P(None, 'tp')
- bias_u: float32 [32, 128], P('tp')
- bias_v: float32 [32, 128], P('tp')
- rel_table: bfloat16 [1024, 4096], replicated
- w_out: bfloat16 [32, 128, 4096], P('tp')
- ffn_gain: float32 [4096], replicated
- w_up: bfloat16 [4096, 16384], P(None, 'tp')
- w_down: bfloat16 [16384, 4096], P('tp')
Outputs:
- output 1: bfloat16 [24, 1024, 4096], P('dp', 'sp')
- output 2: bfloat16 [24, 32, 1024, 128], P(('dp', 'sp'), 'tp')
- output 3: bfloat16 [24, 32, 1024, 128], P(('dp', 'sp'), 'tp')
All inputs are finite; a program needn't handle non-finite values.
Results may differ from the reference program's by a relative error of at most 0.0135117.
Values are sent between devices in bfloat16 or wider.
A program may use at most 1 GiB of HBM per device.

```python
import jax
import jax.numpy as jnp
from jax import lax

BATCH = 24
SEQ_LEN = 1024
D_MODEL = 4096
HEADS = 32
HEAD_DIM = 128
FF_DIM = 16384
QUERY_BLOCK = 128


def rms_norm(values, gain):
    vals_f32 = values.astype(jnp.float32)
    inv_rms = lax.rsqrt(jnp.mean(vals_f32 * vals_f32, axis=-1, keepdims=True) + 1e-6)
    return (vals_f32 * inv_rms * gain).astype(jnp.bfloat16)


def setup_inputs(seed: int = 0, part: int = 0) -> dict:
    key_list = jax.random.split(jax.random.key(seed), 11)
    inner_dim = HEADS * HEAD_DIM
    tokens = jax.random.normal(jax.random.fold_in(key_list[0], part), (BATCH, SEQ_LEN, D_MODEL), jnp.float32)
    attn_gain = 1.0 + 0.25 * jax.random.normal(key_list[1], (D_MODEL,), jnp.float32)
    qkv_scale = jnp.array([1.5, 1.0, 1.0], jnp.float32)[None, :, None, None] * D_MODEL ** -0.5
    w_qkv = jax.random.normal(key_list[2], (D_MODEL, 3, HEADS, HEAD_DIM), jnp.float32) * qkv_scale
    w_rel = jax.random.normal(key_list[3], (D_MODEL, HEADS, HEAD_DIM), jnp.float32) * D_MODEL ** -0.5
    bias_u = jax.random.normal(key_list[4], (HEADS, HEAD_DIM), jnp.float32)
    bias_v = jax.random.normal(key_list[5], (HEADS, HEAD_DIM), jnp.float32)
    rel_table = jax.random.normal(key_list[6], (SEQ_LEN, D_MODEL), jnp.float32)
    w_out = jax.random.normal(key_list[7], (HEADS, HEAD_DIM, D_MODEL), jnp.float32) * inner_dim ** -0.5
    ffn_gain = 1.0 + 0.25 * jax.random.normal(key_list[8], (D_MODEL,), jnp.float32)
    w_up = jax.random.normal(key_list[9], (D_MODEL, FF_DIM), jnp.float32) * D_MODEL ** -0.5
    w_down = jax.random.normal(key_list[10], (FF_DIM, D_MODEL), jnp.float32) * FF_DIM ** -0.5
    return {'tokens': tokens.astype(jnp.bfloat16), 'attn_gain': attn_gain, 'w_qkv': w_qkv.astype(jnp.bfloat16), 'w_rel': w_rel.astype(jnp.bfloat16), 'bias_u': bias_u, 'bias_v': bias_v, 'rel_table': rel_table.astype(jnp.bfloat16), 'w_out': w_out.astype(jnp.bfloat16), 'ffn_gain': ffn_gain, 'w_up': w_up.astype(jnp.bfloat16), 'w_down': w_down.astype(jnp.bfloat16)}


def block_attention(qu_blk, qv_blk, key_rows, val_rows, prev_pad, q_start):
    n_q = qu_blk.shape[1]
    win_len = SEQ_LEN + n_q
    window = lax.dynamic_slice_in_dim(prev_pad, SEQ_LEN - q_start - n_q, win_len, axis=1)
    content = jnp.einsum('hqe,hke->hqk', qu_blk.astype(jnp.float32), key_rows.astype(jnp.float32))
    pos_raw = jnp.einsum('hqe,hle->hql', qv_blk.astype(jnp.float32), window.astype(jnp.float32))
    pos_flat = pos_raw.reshape(HEADS, n_q * win_len)
    pos_term = pos_flat[:, n_q - 1:n_q - 1 + n_q * (win_len - 1)].reshape(HEADS, n_q, win_len - 1)[:, :, :SEQ_LEN]
    scores = (content + pos_term) * HEAD_DIM ** -0.5
    causal = jnp.arange(SEQ_LEN)[None, :] <= (q_start + jnp.arange(n_q))[:, None]
    scores = jnp.where(causal[None], scores, -1e30)
    exp_scores = jnp.exp(scores - jnp.max(scores, axis=-1, keepdims=True))
    row_sum = jnp.sum(exp_scores, axis=-1, keepdims=True)
    weighted = jnp.einsum('hqk,hke->hqe', exp_scores.astype(jnp.bfloat16).astype(jnp.float32), val_rows.astype(jnp.float32))
    return (weighted / row_sum).astype(jnp.bfloat16)


def reference(tokens, attn_gain, w_qkv, w_rel, bias_u, bias_v, rel_table, w_out, ffn_gain, w_up, w_down):
    rel_pos = jnp.einsum('sd,dhe->hse', rel_table.astype(jnp.float32), w_rel.astype(jnp.float32)).astype(jnp.bfloat16)
    prev_pad = jnp.concatenate([jnp.flip(rel_pos, axis=1), jnp.zeros_like(rel_pos)], axis=1)
    qkv_f32 = w_qkv.astype(jnp.float32)
    out_f32 = w_out.astype(jnp.float32)
    block_starts = jnp.arange(SEQ_LEN // QUERY_BLOCK) * QUERY_BLOCK

    def one_prompt(prompt):
        normed = rms_norm(prompt, attn_gain)
        qkv = jnp.einsum('sd,dche->chse', normed.astype(jnp.float32), qkv_f32).astype(jnp.bfloat16)
        query_rows = qkv[0].astype(jnp.float32)
        q_u = (query_rows + bias_u[:, None, :]).astype(jnp.bfloat16)
        q_v = (query_rows + bias_v[:, None, :]).astype(jnp.bfloat16)

        def one_block(q_start):
            qu_blk = lax.dynamic_slice_in_dim(q_u, q_start, QUERY_BLOCK, axis=1)
            qv_blk = lax.dynamic_slice_in_dim(q_v, q_start, QUERY_BLOCK, axis=1)
            return block_attention(qu_blk, qv_blk, qkv[1], qkv[2], prev_pad, q_start)

        blocks = lax.map(one_block, block_starts)
        attn_proj = jnp.einsum('bhqe,hed->bqd', blocks.astype(jnp.float32), out_f32)
        attn_proj = attn_proj.reshape(SEQ_LEN, D_MODEL).astype(jnp.bfloat16)
        hidden = (prompt.astype(jnp.float32) + attn_proj.astype(jnp.float32)).astype(jnp.bfloat16)
        normed_ffn = rms_norm(hidden, ffn_gain)
        up_proj = jax.nn.gelu(jnp.dot(normed_ffn, w_up, preferred_element_type=jnp.float32)).astype(jnp.bfloat16)
        down_proj = jnp.dot(up_proj, w_down, preferred_element_type=jnp.float32).astype(jnp.bfloat16)
        hidden_out = (hidden.astype(jnp.float32) + down_proj.astype(jnp.float32)).astype(jnp.bfloat16)
        return hidden_out, qkv[1], qkv[2]

    hidden_out, k_cache, v_cache = lax.map(one_prompt, tokens)
    return hidden_out, k_cache, v_cache
```

```python
import functools

import jax
import jax.numpy as jnp
from jax import lax
from jax.experimental import pallas as pl
from jax.experimental.pallas import tpu as pltpu
from jax.sharding import PartitionSpec as P


def rms_norm(values, gain):
    vals_f32 = values.astype(jnp.float32)
    inv_rms = lax.rsqrt(jnp.mean(vals_f32 * vals_f32, axis=-1, keepdims=True) + 1e-6)
    return (vals_f32 * inv_rms * gain).astype(jnp.bfloat16)


def attention_kernel(q_ref, k_ref, v_ref, pos_ref, u_ref, w_ref, o_ref, kc_ref, vc_ref):
    n_blk, blk, head_dim = q_ref.shape
    seq = n_blk * blk
    kc_ref[...] = k_ref[...].reshape(seq, head_dim)
    vc_ref[...] = v_ref[...].reshape(seq, head_dim)
    contract_last = (((1,), (1,)), ((), ()))
    rows = lax.broadcasted_iota(jnp.int32, (blk, blk), 0)
    cols = lax.broadcasted_iota(jnp.int32, (blk, blk), 1)
    for idx in range(n_blk):
        keys = (idx + 1) * blk
        width = keys + blk
        query = q_ref[idx].astype(jnp.float32)
        q_u = (query + u_ref[...]).astype(jnp.bfloat16)
        q_v = (query + w_ref[...]).astype(jnp.bfloat16)
        content = lax.dot_general(q_u, kc_ref[pl.ds(0, keys), :], contract_last, preferred_element_type=jnp.float32)
        raw = lax.dot_general(q_v, pos_ref[pl.ds(seq - keys, width), :], contract_last, preferred_element_type=jnp.float32)
        pos_term = pltpu.roll(raw, width - (blk - 1), 1, stride=1, stride_axis=0)[:, :keys]
        scores = (content + pos_term) * (head_dim ** -0.5)
        diag = jnp.where(cols <= rows, scores[:, keys - blk:], -1e30)
        scores = diag if idx == 0 else jnp.concatenate([scores[:, :keys - blk], diag], axis=1)
        exp_scores = jnp.exp(scores - jnp.max(scores, axis=-1, keepdims=True))
        row_sum = jnp.sum(exp_scores, axis=-1, keepdims=True)
        weighted = jnp.dot(exp_scores.astype(jnp.bfloat16), vc_ref[pl.ds(0, keys), :], preferred_element_type=jnp.float32)
        o_ref[idx] = (weighted / row_sum).astype(jnp.bfloat16)


def attention(qkv, pos_pad, bias_u, bias_v):
    n_blk, _, prompts, heads, blk, head_dim = qkv.shape
    seq = n_blk * blk

    def part(which):
        return pl.BlockSpec((n_blk, None, None, None, blk, head_dim), lambda p, h: (0, which, p, h, 0, 0))

    bias_spec = pl.BlockSpec((None, 1, head_dim), lambda p, h: (h, 0, 0))
    cache_spec = pl.BlockSpec((None, None, seq, head_dim), lambda p, h: (p, h, 0, 0))
    cache_shape = jax.ShapeDtypeStruct((prompts, heads, seq, head_dim), jnp.bfloat16)
    flops = prompts * heads * seq * seq * head_dim * 4
    return pl.pallas_call(
        attention_kernel,
        grid=(prompts, heads),
        in_specs=[part(0), part(1), part(2),
                  pl.BlockSpec((None, seq + blk, head_dim), lambda p, h: (h, 0, 0)), bias_spec, bias_spec],
        out_specs=[pl.BlockSpec((n_blk, None, blk, head_dim), lambda p, h: (0, p, 0, h)), cache_spec, cache_spec],
        out_shape=[jax.ShapeDtypeStruct((n_blk, prompts, blk, heads * head_dim), jnp.bfloat16), cache_shape, cache_shape],
        cost_estimate=pl.CostEstimate(flops=flops, bytes_accessed=16 << 20, transcendentals=prompts * heads * seq * seq // 2),
        name="attention",
    )(qkv, qkv, qkv, pos_pad, bias_u[:, None, :], bias_v[:, None, :])


def solution(mesh):
    groups = mesh.shape['sp']
    cols = mesh.shape['tp']

    def shift(value, step):
        return lax.ppermute(value, 'sp', [(i, (i + step) % groups) for i in range(groups)])

    def plane_shift(value, axis, step):
        side = 4
        pairs = []
        for i in range(cols):
            z, y = divmod(i, side)
            pairs.append((i, (z + step) % side * side + y if axis == 0 else z * side + (y + step) % side))
        return lax.ppermute(value, 'tp', pairs)

    def line_gather(value, axis):
        half = value.shape[0] // 2
        nxt = plane_shift(value, axis, -1)
        prv = plane_shift(value, axis, 1)
        return value, nxt, prv, plane_shift(nxt[:half], axis, -1), plane_shift(prv[half:], axis, 1)

    def put(array, value, starts):
        return lax.dynamic_update_slice(array, value, starts)

    def swap(value):
        return lax.ppermute(value, 'sp', [(i, i ^ 1) for i in range(groups)])

    def local_layer(tokens, attn_gain, w_qkv, w_rel, bias_u, bias_v, rel_table, w_out, ffn_gain, w_up, w_down):
        prompts, blk_len, d_model = tokens.shape
        n_heads, head_dim = bias_u.shape
        s_idx = lax.axis_index('sp')
        t_idx = lax.axis_index('tp')
        core = s_idx % 2
        own = prompts // groups
        rows = prompts * blk_len // cols
        ff_cut = w_up.shape[1] // groups

        wo_half = lax.dynamic_index_in_dim(w_out, core, axis=0, keepdims=False)
        w1_cut = lax.dynamic_slice_in_dim(w_up, s_idx * ff_cut, ff_cut, axis=1).T
        first_all = lax.all_gather(jnp.stack([wo_half, w1_cut], axis=0), 'tp', axis=0, tiled=False)
        w2_cut = lax.dynamic_slice_in_dim(w_down, s_idx * ff_cut, ff_cut, axis=0)
        w2_all = lax.all_gather(w2_cut, 'tp', axis=0, tiled=True)

        normed = rms_norm(tokens, attn_gain)
        qkv = jnp.einsum('bsd,dche->cbhse', normed, w_qkv, preferred_element_type=jnp.float32).astype(jnp.bfloat16)
        qkv = qkv.reshape(3, groups, own, n_heads, blk_len, head_dim).transpose(1, 0, 2, 3, 4, 5)
        qkv = lax.all_to_all(qkv, 'sp', split_axis=0, concat_axis=0, tiled=True)
        rel_pos = jnp.einsum('sd,dhe->hse', rel_table, w_rel, preferred_element_type=jnp.float32).astype(jnp.bfloat16)
        pos_pad = jnp.pad(jnp.flip(rel_pos, axis=1), ((0, 0), (0, blk_len), (0, 0)))
        out, k_cache, v_cache = attention(qkv, pos_pad, bias_u, bias_v)

        out = lax.all_to_all(out, 'sp', split_axis=0, concat_axis=0, tiled=True)
        out = out.reshape(cols, rows, n_heads * head_dim)
        out = lax.all_to_all(out, 'tp', split_axis=0, concat_axis=0, tiled=True)
        out = out.reshape(cols, rows, n_heads, head_dim).transpose(2, 1, 0, 3).reshape(n_heads, rows, cols * head_dim)
        out_keep = lax.dynamic_index_in_dim(out, core, axis=0, keepdims=False)
        out_give = lax.dynamic_index_in_dim(out, 1 - core, axis=0, keepdims=False)
        lhs = jnp.concatenate([out_keep, swap(out_give)], axis=0)
        first_all, lhs = lax.optimization_barrier((first_all, lhs))
        wo_own = first_all[:, 0].reshape(cols * head_dim, d_model)
        w1_all = first_all[:, 1].reshape(cols * ff_cut, d_model)
        both = jnp.dot(lhs, wo_own, preferred_element_type=jnp.float32)
        from_core = swap(both[rows:].astype(jnp.bfloat16))
        attn_proj = (both[:rows] + from_core.astype(jnp.float32)).astype(jnp.bfloat16)
        resid = lax.dynamic_slice_in_dim(tokens.reshape(prompts * blk_len, d_model), t_idx * rows, rows, axis=0)
        hidden = (resid.astype(jnp.float32) + attn_proj.astype(jnp.float32)).astype(jnp.bfloat16)
        n_own = rms_norm(hidden, ffn_gain)

        def add(a, b):
            return (a.astype(jnp.float32) + b.astype(jnp.float32)).astype(jnp.bfloat16)

        def up_proj(block):
            up = jnp.einsum('rd,fd->rf', block, w1_all, preferred_element_type=jnp.float32)
            return jax.nn.gelu(up).astype(jnp.bfloat16)

        def down_part(up):
            return jnp.dot(up, w2_all, preferred_element_type=jnp.float32).astype(jnp.bfloat16)

        half = rows // 2
        n_next, n_prev = shift(n_own, -2), shift(n_own, 2)
        t_own = swap(n_own)
        far_a, far_b = shift(n_next[:half], -2), shift(n_prev[half:], 2)
        near = jnp.concatenate([n_next, n_prev], axis=0)
        t_near = swap(near)
        far = jnp.concatenate([far_a, far_b], axis=0)
        t_far = swap(far)
        up_own = up_proj(jnp.concatenate([n_own, t_own], axis=0))
        up_near = up_proj(near)
        up_t_near = up_proj(t_near)
        up_far = up_proj(jnp.concatenate([far, t_far], axis=0))

        give = down_part(jnp.concatenate([up_far[rows:], up_t_near, up_own[rows:]], axis=0))
        part = add(down_part(jnp.concatenate([up_far[:rows], up_near, up_own[:rows]], axis=0)), swap(give))
        p_far, p_next, p_prev, p_own = (part[k * rows:(k + 1) * rows] for k in range(4))
        far_a, far_b = shift(p_far[:half], 2), shift(p_far[half:], -2)
        p_next = jnp.concatenate([add(p_next[:half], far_a), p_next[half:]], axis=0)
        p_prev = jnp.concatenate([p_prev[:half], add(p_prev[half:], far_b)], axis=0)
        r_next, r_prev = shift(p_next, 2), shift(p_prev, -2)
        down_proj = (p_own.astype(jnp.float32) + r_next.astype(jnp.float32) + r_prev.astype(jnp.float32)).astype(jnp.bfloat16)
        y_rows = add(hidden, down_proj)

        z_idx, y_idx = t_idx // 4, t_idx % 4
        y = jnp.zeros((4, 4, 2, half, d_model), jnp.bfloat16)
        for side in range(2):
            piece = y_rows[side * half:(side + 1) * half]
            one, two = (z_idx, y_idx) if side == 0 else (y_idx, z_idx)
            own_p, nxt, prv, far_a, far_b = line_gather(piece, side)
            line = jnp.zeros((4, half, d_model), jnp.bfloat16)
            line = put(line, own_p[None], (one, 0, 0))
            line = put(line, nxt[None], ((one + 1) % 4, 0, 0))
            line = put(line, prv[None], ((one + 3) % 4, 0, 0))
            line = put(line, far_a[None], ((one + 2) % 4, 0, 0))
            line = put(line, far_b[None], ((one + 2) % 4, half // 2, 0))
            own_p, nxt, prv, far_a, far_b = line_gather(line, 1 - side)

            def place(array, value, pos, first):
                if side == 0:
                    return put(array, value[:, None, None], (first, pos % 4, side, 0, 0))
                return put(array, value[None, :, None], (pos % 4, first, side, 0, 0))

            y = place(y, own_p, two, 0)
            y = place(y, nxt, two + 1, 0)
            y = place(y, prv, two + 3, 0)
            y = place(y, far_a, two + 2, 0)
            y = place(y, far_b, two + 2, 2)
        return y.reshape(prompts, blk_len, d_model), k_cache, v_cache

    seq_spec = P('dp', 'sp', None)
    cache_spec = P(('dp', 'sp'), 'tp', None, None)
    in_specs = (seq_spec, P(None), P(None, None, 'tp', None), P(None, 'tp', None), P('tp', None), P('tp', None), P(None, None), P('tp', None, None), P(None), P(None, 'tp'), P('tp', None))
    return jax.shard_map(local_layer, mesh=mesh, in_specs=in_specs, out_specs=(seq_spec, cache_spec, cache_spec), check_vma=False)
```
